128 devices in a mesh: ep: 4 (over z), fsdp: 32 (over y, x, core).
Axes of the slice: x: 4, y: 4, z: 4, core: 2. Of those that a mesh axis runs over, the one named last changes fastest.
Arguments:
- train_gate: float32 [64, 2048, 1408], P('ep', 'fsdp'), may hold values from -0.25 to 0.25
- train_up: float32 [64, 2048, 1408], P('ep', 'fsdp'), may hold values from -0.25 to 0.25
- train_down: float32 [64, 1408, 2048], P('ep', None, 'fsdp'), may hold values from -0.3125 to 0.3125
- router_weight: float32 [2048, 64], P('fsdp', 'ep'), may hold values from -0.125 to 0.125
- router_gain: float32 [2048], P('fsdp'), may hold values from 0.25 to 1.75
Outputs:
- ready_gate: bfloat16 [64, 2048, 1408], P('ep', None, 'fsdp')
- ready_up: bfloat16 [64, 2048, 1408], P('ep', None, 'fsdp')
- ready_down: bfloat16 [64, 1408, 2048], P('ep', 'fsdp')
- scale_gate: float32 [64, 1408], P('ep', 'fsdp')
- scale_up: float32 [64, 1408], P('ep', 'fsdp')
- scale_down: float32 [64, 1408], P('ep', 'fsdp')
- serve_router: bfloat16 [2048, 64], replicated
The draws below stay inside these ranges and needn't reach their ends.
All inputs are finite; a program needn't handle non-finite values.
Results may differ from the reference program's by a relative error of at most 0.001.
Values may be sent and summed in bfloat16 or wider, within the bound.
A program may use at most 192 MiB of HBM per device.

```python
import jax
import jax.numpy as jnp
from jax import lax

EXPERTS = 64
D_MODEL = 2048
D_EXPERT = 1408


def strengthened(drawn, own_key, source, target, shards_of, factor):
    owner, partner = [(jnp.arange(drawn.shape[axis_at]) // (drawn.shape[axis_at] // shards_of)).reshape([-1 if axis == axis_at else 1 for axis in range(drawn.ndim)]) for axis_at in (source, target)]
    chosen = jax.random.permutation(own_key, shards_of)[partner]
    strong = (owner == chosen) | (owner == (partner + shards_of // 2) % shards_of)
    return jnp.where(strong, factor * drawn, drawn)


def block_scale(rng, extent, cuts, smallest, largest):
    gain, own = 1.0, jax.random.fold_in(rng, 6)
    for axis_at, blocks in cuts:
        steps = jnp.exp(jax.random.uniform(jax.random.fold_in(own, axis_at), (blocks,), jnp.float32, smallest / len(cuts), largest / len(cuts)))
        gain = gain * jnp.repeat(steps, extent[axis_at] // blocks).reshape([-1 if axis == axis_at else 1 for axis in range(len(extent))])
    return gain


def normal_values(rng, extent, width, reach, pieces=(), dtype=jnp.bfloat16):
    loudness = block_scale(rng, extent, pieces, -0.22, 0.18) if pieces else 1.0
    result = jax.random.normal(rng, extent, jnp.float32) * width * loudness
    return jnp.minimum(jnp.maximum(result, -reach), reach).astype(dtype)


def bell_draw_with(own_key, dims, width, reach, shards, heavy, held_as=jnp.bfloat16):
    values = width * jax.random.normal(own_key, dims, jnp.float32)
    if shards:
        values = values * block_scale(own_key, dims, shards, -0.22, 0.18)
    return jnp.clip(strengthened(values, jax.random.fold_in(own_key, 3), *heavy), -reach, reach).astype(held_as)


def setup_inputs(seed: int = 0) -> dict:
    seeds = jax.random.split(jax.random.key(seed), 6)
    return {
        "train_gate": bell_draw_with(seeds[0], (EXPERTS, D_MODEL, D_EXPERT), D_MODEL ** -0.5, 0.25, ((0, 4), (1, 32)), (1, 2, 32, 2.75), jnp.float32),
        "train_up": bell_draw_with(seeds[1], (EXPERTS, D_MODEL, D_EXPERT), D_MODEL ** -0.5, 0.25, ((0, 4), (1, 32)), (1, 2, 32, 2.75), jnp.float32),
        "train_down": bell_draw_with(seeds[2], (EXPERTS, D_EXPERT, D_MODEL), D_EXPERT ** -0.5, 0.3125, ((0, 4), (2, 32)), (2, 1, 32, 2.75), jnp.float32),
        "router_weight": normal_values(seeds[3], (D_MODEL, EXPERTS), D_MODEL ** -0.5, 0.125, ((0, 32), (1, 4)), jnp.float32),
        "router_gain": jnp.clip(1.0 + 0.15 * jax.random.normal(seeds[4], (D_MODEL,), jnp.float32), 0.25, 1.75),
    }


def reference(train_gate, train_up, train_down, router_weight, router_gain):
    scale_gate = jnp.sqrt(lax.optimization_barrier(jnp.sum(train_gate * train_gate, axis=1)))
    ready_gate = (train_gate / jnp.expand_dims(scale_gate, 1)).astype(jnp.bfloat16)
    scale_up = jnp.sqrt(lax.optimization_barrier(jnp.sum(train_up * train_up, axis=1)))
    ready_up = (train_up / jnp.expand_dims(scale_up, 1)).astype(jnp.bfloat16)
    scale_down = jnp.sqrt(lax.optimization_barrier(jnp.sum(train_down * train_down, axis=2)))
    ready_down = (train_down / jnp.expand_dims(scale_down, 2)).astype(jnp.bfloat16)
    serve_router = (router_weight * router_gain[:, None]).astype(jnp.bfloat16)
    return (ready_gate, ready_up, ready_down, scale_gate, scale_up, scale_down, serve_router)
```

```python
import functools

import jax
import jax.numpy as jnp
from jax import lax
from jax.experimental import pallas as pl
from jax.experimental.pallas import tpu as pltpu
from jax.sharding import PartitionSpec as P

MESH = pl.DeviceIdType.MESH
F32, BF16 = jnp.float32, jnp.bfloat16

NX, NY, NZ = 4, 4, 4
EXP, ROWS, COLS = 16, 64, 1408
HALF = EXP // 2
PIECE = COLS // 32
TILES = COLS // 128
OFFS = [(dx, dy) for dy in range(NY) for dx in range(NX) if (dx, dy) != (0, 0)]
GROUP = 512


def exchange(
    gate, up, down, rw, gain,
    out_g, out_u, out_d, sc_g, sc_u, sc_d, rout,
    xf, xo, psum, rsbuf, myscl, scal, scal_o, tr, sb, big, rhalf, rbuf,
    lsem, osem, dsem_s, dsem_r, rs_s, rs_r, ag_s, ag_r, fw_s, fw_r, bk_s, bk_r,
    rt_s, rt_r,
):
    srcs, outs, scs = (gate, up, down), (out_g, out_u, out_d), (sc_g, sc_u, sc_d)
    f = lax.axis_index("fsdp")
    z = lax.axis_index("ep")
    core = lax.rem(f, 2)
    chip = lax.div(f, 2)
    x, y = lax.rem(chip, NX), lax.div(chip, NX)

    def chip_at(dx, dy):
        return lax.rem(y + dy, NY) * NX + lax.rem(x + dx, NX)

    def local(m, e):
        return pltpu.make_async_copy(
            srcs[m].at[core * HALF + e], xf.at[m, e, core], lsem.at[m, e])

    def other(e):
        return pltpu.make_async_copy(
            srcs[0].at[(1 - core) * HALF + e], xo.at[e], osem.at[e])

    def send(src, dst, ss, rs, dev):
        pltpu.make_async_remote_copy(
            src_ref=src, dst_ref=dst, send_sem=ss, recv_sem=rs,
            device_id={"fsdp": dev}, device_id_type=MESH).start()

    def await_bytes(ref, sem):
        pltpu.make_async_copy(ref, ref, sem).wait()

    for e in range(HALF):
        local(0, e).start()
        other(e).start()
    for m in (1, 2):
        for e in range(HALF):
            local(m, e).start()

    bar = pltpu.get_barrier_semaphore()
    for c in range(2):
        for dx, dy in OFFS:
            pl.semaphore_signal(bar, inc=1, device_id={"fsdp": chip_at(dx, dy) * 2 + c}, device_id_type=MESH)
    pl.semaphore_signal(bar, inc=1, device_id={"fsdp": f + 1 - 2 * core}, device_id_type=MESH)
    for dz in range(1, NZ):
        pl.semaphore_signal(bar, inc=1, device_id={"ep": lax.rem(z + dz, NZ)}, device_id_type=MESH)
    pl.semaphore_wait(bar, 31 + NZ - 1)

    mate = f + 1 - 2 * core
    for m in range(3):
        for e in range(HALF):
            send(srcs[m].at[(1 - core) * HALF + e], xf.at[m, e, core], dsem_s.at[m, e], dsem_r.at[m, e], mate)

    for k in range(4):
        psum[k, :, TILES] = jnp.ones((HALF, 1, 128), F32)

    def total_rows(parts, row):
        s = None
        for p in parts:
            q = jnp.sum(p * p, axis=0, keepdims=True)
            s = q if s is None else s + q
        for t in range(TILES):
            psum[row[0], row[1], t] = s[:, t * 128:(t + 1) * 128]

    def sums0(e, carry):
        local(0, e).wait()
        total_rows([xf[0, e, core]], (0, e))
        other(e).wait()
        total_rows([xo[e]], (3, e))
        return carry

    def sums(m, e, carry):
        local(m, e).wait()
        await_bytes(xf.at[m, e, 0], dsem_r.at[m, e])
        total_rows([xf[m, e, 0], xf[m, e, 1]], (m, e))
        return carry

    BASE = (0, 31, 46)

    def part(k, c):
        return psum.at[k, lax.div(c, 2), pl.ds(6 * lax.rem(c, 2), 6)]

    def rs_send(m):
        for k, (dx, dy) in enumerate(OFFS):
            c = chip_at(dx, dy)
            send(part(m, c), rsbuf.at[BASE[m] + k], rs_s.at[m], rs_r.at[m], c * 2 + core)
            if m == 0:
                send(part(3, c), rsbuf.at[15 + k], rs_s.at[m], rs_r.at[m], c * 2 + 1 - core)
        if m == 0:
            send(part(3, chip), rsbuf.at[30], rs_s.at[m], rs_r.at[m], mate)

    def ag_send(m):
        n = 31 if m == 0 else 15
        mine = rsbuf.at[pl.ds(BASE[m], n)]
        await_bytes(mine, rs_r.at[m])
        s = psum[m, lax.div(chip, 2), pl.ds(6 * lax.rem(chip, 2), 6)]
        for k in range(n):
            s = s + rsbuf[BASE[m] + k]
        s = jnp.sqrt(s)
        myscl[m] = s
        spot = scal.at[m, lax.div(chip, 2), pl.ds(6 * lax.rem(chip, 2), 6)]
        for dx, dy in OFFS:
            send(myscl.at[m], spot, ag_s.at[m], ag_r.at[m], chip_at(dx, dy) * 2 + core)
        scal[m, lax.div(chip, 2), pl.ds(6 * lax.rem(chip, 2), 6)] = s

    def ag_wait(m):
        await_bytes(rsbuf.at[pl.ds(0, 15)], ag_r.at[m])
        send(scal.at[m], scal_o.at[m], fw_s.at[m], fw_r.at[m], mate)

    def bulk(m, dy):
        row = lax.rem(y + dy, NY)
        first = jnp.minimum(lax.div(row * 352, 128), TILES - 4)
        slot = (m * 4 + dy) * GROUP

        def one(t, carry):
            tile = first + t
            lanes = pl.ds(pl.multiple_of(tile * 128, 128), 128)
            for e in range(HALF):
                inv = 1.0 / scal[m, e, tile]
                blk = jnp.concatenate([xf[m, e, 0, :, lanes], xf[m, e, 1, :, lanes]], axis=0)
                tr[pl.ds(e, 128, stride=8), :] = (blk * inv).T
            v = tr[...].reshape(128, 8, 128).astype(BF16)
            sb[pl.ds(slot + t * 128, 128)] = v
            return carry

        lax.fori_loop(0, 4, one, 0)
        for dx in (1, 3, 2, 0):
            for c in range(2):
                to = (row * NX + lax.rem(x + dx, NX)) * 2
                if dx == 0 and dy == 0:
                    if c == 1:
                        continue
                    to = mate
                else:
                    to = to + c
                at = slot + to * PIECE - first * 128
                send(
                    sb.at[pl.ds(at, PIECE)],
                    outs[m].at[:, pl.ds(pl.multiple_of(core * 8, 8), 8), pl.ds(pl.multiple_of(chip * 128, 128), 128)],
                    bk_s.at[m], bk_r.at[m], to)
        if dy == 0:
            at = slot + f * PIECE - first * 128
            lanes = pl.ds(pl.multiple_of(chip * 128, 128), 128)
            for c in range(2):
                @pl.when(core == c)
                def _():
                    def put(j, carry):
                        outs[m][j, 8 * c:8 * c + 8, lanes] = sb[at + j]
                        return carry
                    lax.fori_loop(0, PIECE, put, 0)

    def route_pair():
        v = rw[...] * gain[...]
        rhalf[0] = jnp.concatenate([v, v], axis=1)
        send(rhalf.at[0], rhalf.at[1], rt_s.at[0], rt_r.at[0], mate)

    def route_plane():
        await_bytes(rhalf.at[1], rt_r.at[0])
        low = lax.broadcasted_iota(jnp.int32, (EXP, 128), 1) < 64
        mine = low == (core == 0)
        rbuf[z, chip] = jnp.where(mine, rhalf[0], rhalf[1]).astype(BF16)
        for dx, dy in OFFS:
            send(rbuf.at[z, chip], rbuf.at[z, chip], rt_s.at[1], rt_r.at[1], chip_at(dx, dy) * 2 + core)

    def route_line():
        await_bytes(rbuf.at[0, pl.ds(0, 15)], rt_r.at[1])
        for dz in range(1, NZ):
            pltpu.make_async_remote_copy(
                src_ref=rbuf.at[z], dst_ref=rbuf.at[z], send_sem=rt_s.at[2], recv_sem=rt_r.at[2],
                device_id={"ep": lax.rem(z + dz, NZ)}, device_id_type=MESH).start()

    def route_out():
        await_bytes(rbuf.at[pl.ds(0, 3)], rt_r.at[2])
        for a in range(NZ):
            for c in range(16):
                rout[a * EXP:(a + 1) * EXP, c * 128:(c + 1) * 128] = rbuf[a, c]

    def scale_out(m):
        await_bytes(scal_o.at[m], fw_r.at[m])
        for e in range(HALF):
            for t in range(TILES + 1):
                own, oth = scal[m, e, t], scal_o[m, e, t]
                big[e:e + 1, t * 128:(t + 1) * 128] = jnp.where(core == 0, own, oth)
                big[HALF + e:HALF + e + 1, t * 128:(t + 1) * 128] = jnp.where(core == 0, oth, own)
        start = f * PIECE
        t0, r = lax.div(start, 128), lax.rem(start, 128)
        a = big[:, pl.ds(pl.multiple_of(t0 * 128, 128), 128)]
        b = big[:, pl.ds(pl.multiple_of(t0 * 128 + 128, 128), 128)]
        shift = lax.rem(128 - r, 128)
        a, b = pltpu.roll(a, shift, 1), pltpu.roll(b, shift, 1)
        lane = lax.broadcasted_iota(jnp.int32, (EXP, 128), 1)
        scs[m][...] = jnp.where(lane < 128 - r, a, b)[:, :PIECE]

    route_pair()
    lax.fori_loop(0, HALF, sums0, 0)
    rs_send(0)
    route_plane()
    ag_send(0)
    lax.fori_loop(0, HALF, functools.partial(sums, 1), 0)
    rs_send(1)
    lax.fori_loop(0, HALF, lambda e, carry: (await_bytes(xf.at[0, e, 0], dsem_r.at[0, e]), carry)[1], 0)
    ag_wait(0)
    bulk(0, 1)
    ag_send(1)
    lax.fori_loop(0, HALF, functools.partial(sums, 2), 0)
    rs_send(2)
    bulk(0, 3)
    route_line()
    bulk(0, 2)
    bulk(0, 0)
    ag_send(2)
    ag_wait(1)
    for dy in (1, 3, 2, 0):
        bulk(1, dy)
    ag_wait(2)
    for dy in (1, 3, 2, 0):
        bulk(2, dy)
    for m in range(3):
        scale_out(m)
    route_out()

    for m in range(3):
        for e in range(HALF):
            await_bytes(xf.at[m, e, 0], dsem_s.at[m, e])
        await_bytes(rsbuf.at[pl.ds(0, 31 if m == 0 else 15)], rs_s.at[m])
        await_bytes(rsbuf.at[pl.ds(0, 15)], ag_s.at[m])
        await_bytes(scal.at[m], fw_s.at[m])
    await_bytes(rhalf.at[0], rt_s.at[0])
    await_bytes(rbuf.at[0, pl.ds(0, 15)], rt_s.at[1])
    await_bytes(rbuf.at[pl.ds(0, 3)], rt_s.at[2])
    for m in range(3):
        await_bytes(sb.at[pl.ds(0, 31 * PIECE)], bk_s.at[m])
        await_bytes(sb.at[pl.ds(0, 31 * PIECE)], bk_r.at[m])


def settle(*refs):
    n = len(refs) // 2
    sem = refs[-1]
    for i in range(n):
        pltpu.make_async_copy(refs[i], refs[n + i], sem.at[i]).start()
    for i in range(n):
        pltpu.make_async_copy(refs[i], refs[n + i], sem.at[i]).wait()


def body(train_gate, train_up, train_down, router_weight, router_gain):
    down = jnp.transpose(train_down, (0, 2, 1))
    shapes = (
        [jax.ShapeDtypeStruct((PIECE, EXP, 2048), BF16)] * 3
        + [jax.ShapeDtypeStruct((EXP, PIECE), F32)] * 3
        + [jax.ShapeDtypeStruct((EXP * NZ, 2048), BF16)]
    )
    vmem = pl.BlockSpec(memory_space=pltpu.VMEM)
    hbm = pl.BlockSpec(memory_space=pl.ANY)
    dma = pltpu.SemaphoreType.DMA
    got = pl.pallas_call(
        exchange,
        out_shape=shapes,
        in_specs=[hbm, hbm, hbm, vmem, vmem],
        out_specs=[vmem] * 7,
        scratch_shapes=[
            pltpu.VMEM((3, HALF, 2, ROWS, COLS), F32),
            pltpu.VMEM((HALF, ROWS, COLS), F32),
            pltpu.VMEM((4, HALF, TILES + 1, 1, 128), F32),
            pltpu.VMEM((61, 6, 1, 128), F32),
            pltpu.VMEM((3, 6, 1, 128), F32),
            pltpu.VMEM((3, HALF, TILES + 1, 1, 128), F32),
            pltpu.VMEM((3, HALF, TILES + 1, 1, 128), F32),
            pltpu.VMEM((1024, 128), F32),
            pltpu.VMEM((12 * GROUP, 8, 128), BF16),
            pltpu.VMEM((EXP, (TILES + 1) * 128), F32),
            pltpu.VMEM((2, EXP, 128), F32),
            pltpu.VMEM((NZ, 16, EXP, 128), BF16),
            dma((3, HALF)), dma((HALF,)), dma((3, HALF)), dma((3, HALF)),
            dma((3,)), dma((3,)), dma((3,)), dma((3,)), dma((3,)), dma((3,)), dma((3,)), dma((3,)),
            dma((3,)), dma((3,)),
        ],
        compiler_params=pltpu.CompilerParams(
            collective_id=0, has_side_effects=True, vmem_limit_bytes=44 * 1024 * 1024
        ),
        name="exchange",
    )(train_gate, train_up, down, router_weight.T, router_gain[None, :])
    done = pl.pallas_call(
        settle,
        out_shape=shapes,
        in_specs=[vmem] * 7,
        out_specs=[hbm] * 7,
        scratch_shapes=[dma((7,))],
        compiler_params=pltpu.CompilerParams(vmem_limit_bytes=2 * 1024 * 1024),
        name="settle",
    )(*got)
    g, u, d, sg, su, sd, r = done
    back = lambda a: jnp.transpose(a, (1, 2, 0))
    return back(g), back(u), jnp.transpose(d, (1, 0, 2)), sg, su, sd, r.T


def solution(mesh):
    return jax.shard_map(
        body,
        mesh=mesh,
        in_specs=(
            P("ep", "fsdp", None),
            P("ep", "fsdp", None),
            P("ep", None, "fsdp"),
            P("fsdp", "ep"),
            P("fsdp"),
        ),
        out_specs=(
            P("ep", None, "fsdp"),
            P("ep", None, "fsdp"),
            P("ep", "fsdp", None),
            P("ep", "fsdp"),
            P("ep", "fsdp"),
            P("ep", "fsdp"),
            P(),
        ),
        check_vma=False,
    )
```

```python
import functools

import jax
import jax.numpy as jnp
from jax import lax
from jax.experimental import pallas as pl
from jax.experimental.pallas import tpu as pltpu
from jax.sharding import PartitionSpec as P

MESH = pl.DeviceIdType.MESH
F32, BF16 = jnp.float32, jnp.bfloat16

NX, NY, NZ = 4, 4, 4
EXP, ROWS, COLS = 16, 64, 1408
HALF = EXP // 2
PIECE = COLS // 32
TILES = COLS // 128
OFFS = sorted([(dx, dy) for dy in range(NY) for dx in range(NX) if (dx, dy) != (0, 0)], key=lambda p: -(min(p[0], 4 - p[0]) + min(p[1], 4 - p[1])))
CUT = 4


def exchange(
    gate, up, down, rw_h, gain_h,
    out_g, out_u, out_d, sc_g, sc_u, sc_d, rout,
    xf, xo, psum, rsbuf, myscl, scal, scal_o, tr, sb, big, rw, gain, rhalf, rbuf,
    isem, lsem, osem, dsem_s, dsem_r, rs_s, rs_r, ag_s, ag_r, fw_s, fw_r, bk_s, bk_r,
    rt_s, rt_r,
):
    srcs, outs, scs = (gate, up, down), (out_g, out_u, out_d), (sc_g, sc_u, sc_d)
    f = lax.axis_index("fsdp")
    z = lax.axis_index("ep")
    core = lax.rem(f, 2)
    chip = lax.div(f, 2)
    x, y = lax.rem(chip, NX), lax.div(chip, NX)

    def chip_at(dx, dy):
        return lax.rem(y + dy, NY) * NX + lax.rem(x + dx, NX)

    def local(m, e):
        return pltpu.make_async_copy(
            srcs[m].at[core * HALF + e], xf.at[m, e, core], lsem.at[m, e])

    def other(m, e):
        return pltpu.make_async_copy(
            srcs[m].at[(1 - core) * HALF + e], xo.at[m, e], osem.at[m, e])

    def send(src, dst, ss, rs, dev):
        pltpu.make_async_remote_copy(
            src_ref=src, dst_ref=dst, send_sem=ss, recv_sem=rs,
            device_id={"fsdp": dev}, device_id_type=MESH).start()

    def await_bytes(ref, sem):
        pltpu.make_async_copy(ref, ref, sem).wait()

    rin = (pltpu.make_async_copy(rw_h, rw, isem.at[0]), pltpu.make_async_copy(gain_h, gain, isem.at[1]))
    for e in range(HALF):
        local(0, e).start()
        other(0, e).start()
    for c in rin:
        c.start()
    for m in (1, 2):
        for e in range(HALF):
            local(m, e).start()
            other(m, e).start()

    bar = pltpu.get_barrier_semaphore()
    for c in range(2):
        for dx, dy in OFFS:
            pl.semaphore_signal(bar, inc=1, device_id={"fsdp": chip_at(dx, dy) * 2 + c}, device_id_type=MESH)
    pl.semaphore_signal(bar, inc=1, device_id={"fsdp": f + 1 - 2 * core}, device_id_type=MESH)
    for dz in range(1, NZ):
        pl.semaphore_signal(bar, inc=1, device_id={"ep": lax.rem(z + dz, NZ)}, device_id_type=MESH)

    mate = f + 1 - 2 * core

    def swap(m, es=range(HALF)):
        for e in es:
            send(xo.at[m, e], xf.at[m, e, core], dsem_s.at[m], dsem_r.at[m], mate)

    for k in range(6):
        psum[k, :, TILES] = jnp.ones((HALF, 1, 128), F32)

    def total_rows(p, k, e):
        s = jnp.sum(p * p, axis=0, keepdims=True)
        for t in range(TILES):
            psum[k, e, t] = s[:, t * 128:(t + 1) * 128]

    def sums(m, e, carry):
        local(m, e).wait()
        total_rows(xf[m, e, core], m, e)
        other(m, e).wait()
        total_rows(xo[m, e], 3 + m, e)
        return carry

    def part(k, c):
        return psum.at[k, lax.div(c, 2), pl.ds(6 * lax.rem(c, 2), 6)]

    def rs_send(m):
        for k, (dx, dy) in enumerate(OFFS):
            c = chip_at(dx, dy)
            send(part(m, c), rsbuf.at[m, k], rs_s.at[m], rs_r.at[m], c * 2 + core)
            send(part(3 + m, c), rsbuf.at[m, 15 + k], rs_s.at[m], rs_r.at[m], c * 2 + 1 - core)
        send(part(3 + m, chip), rsbuf.at[m, 30], rs_s.at[m], rs_r.at[m], mate)

    def ag_send(m):
        await_bytes(rsbuf.at[m], rs_r.at[m])
        s = psum[m, lax.div(chip, 2), pl.ds(6 * lax.rem(chip, 2), 6)]
        for k in range(31):
            s = s + rsbuf[m, k]
        s = jnp.sqrt(s)
        myscl[m] = s
        spot = scal.at[m, lax.div(chip, 2), pl.ds(6 * lax.rem(chip, 2), 6)]
        for dx, dy in OFFS:
            send(myscl.at[m], spot, ag_s.at[m], ag_r.at[m], chip_at(dx, dy) * 2 + core)
        scal[m, lax.div(chip, 2), pl.ds(6 * lax.rem(chip, 2), 6)] = s

    def ag_wait(m):
        await_bytes(rsbuf.at[0, pl.ds(0, 15)], ag_r.at[m])
        send(scal.at[m], scal_o.at[m], fw_s.at[m], fw_r.at[m], mate)

    def fill(m):
        def one(t, carry):
            lanes = pl.ds(pl.multiple_of(t * 128, 128), 128)
            for e in range(HALF):
                inv = 1.0 / scal[m, e, t]
                blk = jnp.concatenate([xf[m, e, 0, :, lanes], xf[m, e, 1, :, lanes]], axis=0)
                tr[pl.ds(e, 128, stride=8), :] = (blk * inv).T
            sb[m, pl.ds(t * 128, 128)] = tr[...].reshape(128, 8, 128).astype(BF16)
            return carry

        lax.fori_loop(0, TILES, one, 0)

    def bulk(m):
        n = PIECE // CUT

        def go(to, h):
            send(
                sb.at[m, pl.ds(to * PIECE + h * n, n)],
                outs[m].at[pl.ds(h * n, n), pl.ds(pl.multiple_of(core * 8, 8), 8), pl.ds(pl.multiple_of(chip * 128, 128), 128)],
                bk_s.at[m], bk_r.at[m], to)

        def turn(h, carry):
            for c in range(2):
                for dx, dy in OFFS:
                    go(chip_at(dx, dy) * 2 + (core if c == 0 else 1 - core), h)
            go(mate, h)
            return carry

        if m == 0:
            for h in range(CUT):
                turn(h, 0)
                swap(1 + h // 2, range(4 * (h % 2), 4 * (h % 2) + 4))
        else:
            lax.fori_loop(0, CUT, turn, 0)
        lanes = pl.ds(pl.multiple_of(chip * 128, 128), 128)
        for c in range(2):
            @pl.when(core == c)
            def _():
                def put(j, carry):
                    outs[m][j, 8 * c:8 * c + 8, lanes] = sb[m, f * PIECE + j]
                    return carry
                lax.fori_loop(0, PIECE, put, 0)

    def route_pair():
        for c in rin:
            c.wait()
        v = rw[...] * gain[...]
        rhalf[0] = jnp.concatenate([v, v], axis=1)
        send(rhalf.at[0], rhalf.at[1], rt_s.at[0], rt_r.at[0], mate)

    def route_plane():
        await_bytes(rhalf.at[1], rt_r.at[0])
        low = lax.broadcasted_iota(jnp.int32, (EXP, 128), 1) < 64
        mine = low == (core == 0)
        rbuf[z, chip] = jnp.where(mine, rhalf[0], rhalf[1]).astype(BF16)
        for dx, dy in OFFS:
            send(rbuf.at[z, chip], rbuf.at[z, chip], rt_s.at[1], rt_r.at[1], chip_at(dx, dy) * 2 + core)

    def route_line():
        await_bytes(rbuf.at[0, pl.ds(0, 15)], rt_r.at[1])
        for dz in range(1, NZ):
            pltpu.make_async_remote_copy(
                src_ref=rbuf.at[z], dst_ref=rbuf.at[z], send_sem=rt_s.at[2], recv_sem=rt_r.at[2],
                device_id={"ep": lax.rem(z + dz, NZ)}, device_id_type=MESH).start()

    def route_out():
        await_bytes(rbuf.at[pl.ds(0, 3)], rt_r.at[2])
        for a in range(NZ):
            for c in range(16):
                rout[a * EXP:(a + 1) * EXP, c * 128:(c + 1) * 128] = rbuf[a, c]

    def scale_out(m):
        await_bytes(scal_o.at[m], fw_r.at[m])
        for e in range(HALF):
            for t in range(TILES + 1):
                own, oth = scal[m, e, t], scal_o[m, e, t]
                big[e:e + 1, t * 128:(t + 1) * 128] = jnp.where(core == 0, own, oth)
                big[HALF + e:HALF + e + 1, t * 128:(t + 1) * 128] = jnp.where(core == 0, oth, own)
        start = f * PIECE
        t0, r = lax.div(start, 128), lax.rem(start, 128)
        a = big[:, pl.ds(pl.multiple_of(t0 * 128, 128), 128)]
        b = big[:, pl.ds(pl.multiple_of(t0 * 128 + 128, 128), 128)]
        shift = lax.rem(128 - r, 128)
        a, b = pltpu.roll(a, shift, 1), pltpu.roll(b, shift, 1)
        lane = lax.broadcasted_iota(jnp.int32, (EXP, 128), 1)
        scs[m][...] = jnp.where(lane < 128 - r, a, b)[:, :PIECE]

    for m in range(3):
        lax.fori_loop(0, HALF, functools.partial(sums, m), 0)
        if m == 0:
            pl.semaphore_wait(bar, 31 + NZ - 1)
        rs_send(m)
        if m == 0:
            swap(0)
    route_pair()
    for m in range(3):
        ag_send(m)
    route_plane()
    for m in range(3):
        ag_wait(m)
        await_bytes(xo.at[m], dsem_r.at[m])
        fill(m)
        bulk(m)
    route_line()
    for m in range(3):
        scale_out(m)
    route_out()

    for m in range(3):
        await_bytes(xo.at[m], dsem_s.at[m])
        await_bytes(rsbuf.at[m], rs_s.at[m])
        await_bytes(rsbuf.at[0, pl.ds(0, 15)], ag_s.at[m])
        await_bytes(scal.at[m], fw_s.at[m])
    await_bytes(rhalf.at[0], rt_s.at[0])
    await_bytes(rbuf.at[0, pl.ds(0, 15)], rt_s.at[1])
    await_bytes(rbuf.at[pl.ds(0, 3)], rt_s.at[2])
    for m in range(3):
        await_bytes(sb.at[m, pl.ds(0, 31 * PIECE)], bk_s.at[m])
        await_bytes(sb.at[m, pl.ds(0, 31 * PIECE)], bk_r.at[m])


def settle(*refs):
    n = len(refs) // 2
    sem = refs[-1]
    for i in range(n):
        pltpu.make_async_copy(refs[i], refs[n + i], sem.at[i]).start()
    for i in range(n):
        pltpu.make_async_copy(refs[i], refs[n + i], sem.at[i]).wait()


def body(train_gate, train_up, train_down, router_weight, router_gain):
    down = jnp.transpose(train_down, (0, 2, 1))
    shapes = (
        [jax.ShapeDtypeStruct((PIECE, EXP, 2048), BF16)] * 3
        + [jax.ShapeDtypeStruct((EXP, PIECE), F32)] * 3
        + [jax.ShapeDtypeStruct((EXP * NZ, 2048), BF16)]
    )
    vmem = pl.BlockSpec(memory_space=pltpu.VMEM)
    hbm = pl.BlockSpec(memory_space=pl.ANY)
    dma = pltpu.SemaphoreType.DMA
    got = pl.pallas_call(
        exchange,
        out_shape=shapes,
        in_specs=[hbm] * 5,
        out_specs=[vmem] * 7,
        scratch_shapes=[
            pltpu.VMEM((3, HALF, 2, ROWS, COLS), F32),
            pltpu.VMEM((3, HALF, ROWS, COLS), F32),
            pltpu.VMEM((6, HALF, TILES + 1, 1, 128), F32),
            pltpu.VMEM((3, 31, 6, 1, 128), F32),
            pltpu.VMEM((3, 6, 1, 128), F32),
            pltpu.VMEM((3, HALF, TILES + 1, 1, 128), F32),
            pltpu.VMEM((3, HALF, TILES + 1, 1, 128), F32),
            pltpu.VMEM((1024, 128), F32),
            pltpu.VMEM((3, COLS, 8, 128), BF16),
            pltpu.VMEM((EXP, (TILES + 1) * 128), F32),
            pltpu.VMEM((EXP, ROWS), F32),
            pltpu.VMEM((1, ROWS), F32),
            pltpu.VMEM((2, EXP, 128), F32),
            pltpu.VMEM((NZ, 16, EXP, 128), BF16),
            dma((2,)), dma((3, HALF)), dma((3, HALF)), *[dma((3,))] * 12,
        ],
        compiler_params=pltpu.CompilerParams(
            collective_id=0, has_side_effects=True, vmem_limit_bytes=44 * 1024 * 1024
        ),
        name="exchange",
    )(train_gate, train_up, down, router_weight.T, router_gain[None, :])
    done = pl.pallas_call(
        settle,
        out_shape=shapes,
        in_specs=[vmem] * 7,
        out_specs=[hbm] * 7,
        scratch_shapes=[dma((7,))],
        compiler_params=pltpu.CompilerParams(vmem_limit_bytes=2 * 1024 * 1024),
        name="settle",
    )(*got)
    g, u, d, sg, su, sd, r = done
    back = lambda a: jnp.transpose(a, (1, 2, 0))
    return back(g), back(u), jnp.transpose(d, (1, 0, 2)), sg, su, sd, r.T


def solution(mesh):
    return jax.shard_map(
        body,
        mesh=mesh,
        in_specs=(
            P("ep", "fsdp", None),
            P("ep", "fsdp", None),
            P("ep", None, "fsdp"),
            P("fsdp", "ep"),
            P("fsdp"),
        ),
        out_specs=(
            P("ep", None, "fsdp"),
            P("ep", None, "fsdp"),
            P("ep", "fsdp", None),
            P("ep", "fsdp"),
            P("ep", "fsdp"),
            P("ep", "fsdp"),
            P(),
        ),
        check_vma=False,
    )
```

```python
import functools

import jax
import jax.numpy as jnp
from jax import lax
from jax.experimental import pallas as pl
from jax.experimental.pallas import tpu as pltpu
from jax.sharding import PartitionSpec as P

MESH = pl.DeviceIdType.MESH
F32, BF16 = jnp.float32, jnp.bfloat16

NX, NY, NZ = 4, 4, 4
EXP, ROWS, COLS = 16, 64, 1408
HALF = EXP // 2
PIECE = COLS // 32
TILES = COLS // 128
OFFS = sorted([(dx, dy) for dy in range(NY) for dx in range(NX) if (dx, dy) != (0, 0)], key=lambda p: -(min(p[0], 4 - p[0]) + min(p[1], 4 - p[1])))
CUT = 4
RAW = 4


def exchange(
    gate, up, down, rw_h, gain_h,
    out_g, out_u, out_d, sc_g, sc_u, sc_d, rout,
    xf, xo, psum, rsbuf, myscl, scal, scal_o, tr, sb, rawsb, rraw, big, rw, gain, rhalf, rbuf,
    isem, lsem, osem, dsem_s, dsem_r, rs_s, rs_r, ag_s, ag_r, fw_s, fw_r, bk_s, bk_r,
    rt_s, rt_r, rw_s, rw_r,
):
    srcs, outs, scs = (gate, up, down), (out_g, out_u, out_d), (sc_g, sc_u, sc_d)
    f = lax.axis_index("fsdp")
    z = lax.axis_index("ep")
    core = lax.rem(f, 2)
    chip = lax.div(f, 2)
    x, y = lax.rem(chip, NX), lax.div(chip, NX)

    def chip_at(dx, dy):
        return lax.rem(y + dy, NY) * NX + lax.rem(x + dx, NX)

    def local(m, e):
        return pltpu.make_async_copy(
            srcs[m].at[core * HALF + e], xf.at[m, e, core], lsem.at[m, e])

    def other(m, e):
        return pltpu.make_async_copy(
            srcs[m].at[(1 - core) * HALF + e], xo.at[m, e], osem.at[m, e])

    def send(src, dst, ss, rs, dev):
        pltpu.make_async_remote_copy(
            src_ref=src, dst_ref=dst, send_sem=ss, recv_sem=rs,
            device_id={"fsdp": dev}, device_id_type=MESH).start()

    def await_bytes(ref, sem):
        pltpu.make_async_copy(ref, ref, sem).wait()

    rin = (pltpu.make_async_copy(rw_h, rw, isem.at[0]), pltpu.make_async_copy(gain_h, gain, isem.at[1]))
    for e in range(HALF):
        local(0, e).start()
        other(0, e).start()
    for c in rin:
        c.start()
    for m in (1, 2):
        for e in range(HALF):
            local(m, e).start()
            other(m, e).start()

    bar = pltpu.get_barrier_semaphore()
    for c in range(2):
        for dx, dy in OFFS:
            pl.semaphore_signal(bar, inc=1, device_id={"fsdp": chip_at(dx, dy) * 2 + c}, device_id_type=MESH)
    pl.semaphore_signal(bar, inc=1, device_id={"fsdp": f + 1 - 2 * core}, device_id_type=MESH)
    for dz in range(1, NZ):
        pl.semaphore_signal(bar, inc=1, device_id={"ep": lax.rem(z + dz, NZ)}, device_id_type=MESH)

    mate = f + 1 - 2 * core

    def swap(m, es=range(HALF)):
        for e in es:
            send(xo.at[m, e], xf.at[m, e, core], dsem_s.at[m], dsem_r.at[m], mate)

    for k in range(6):
        psum[k, :, TILES] = jnp.ones((HALF, 1, 128), F32)

    def total_rows(p, k, e):
        s = jnp.sum(p * p, axis=0, keepdims=True)
        for t in range(TILES):
            psum[k, e, t] = s[:, t * 128:(t + 1) * 128]

    def sums(m, e, carry):
        local(m, e).wait()
        total_rows(xf[m, e, core], m, e)
        other(m, e).wait()
        total_rows(xo[m, e], 3 + m, e)
        return carry

    def part(k, c):
        return psum.at[k, lax.div(c, 2), pl.ds(6 * lax.rem(c, 2), 6)]

    def rs_send(m):
        for k, (dx, dy) in enumerate(OFFS):
            c = chip_at(dx, dy)
            send(part(m, c), rsbuf.at[m, k], rs_s.at[m], rs_r.at[m], c * 2 + core)
            send(part(3 + m, c), rsbuf.at[m, 15 + k], rs_s.at[m], rs_r.at[m], c * 2 + 1 - core)
        send(part(3 + m, chip), rsbuf.at[m, 30], rs_s.at[m], rs_r.at[m], mate)

    def ag_send(m):
        await_bytes(rsbuf.at[m], rs_r.at[m])
        s = psum[m, lax.div(chip, 2), pl.ds(6 * lax.rem(chip, 2), 6)]
        for k in range(31):
            s = s + rsbuf[m, k]
        s = jnp.sqrt(s)
        myscl[m] = s
        spot = scal.at[m, lax.div(chip, 2), pl.ds(6 * lax.rem(chip, 2), 6)]
        for dx, dy in OFFS:
            send(myscl.at[m], spot, ag_s.at[m], ag_r.at[m], chip_at(dx, dy) * 2 + core)
        scal[m, lax.div(chip, 2), pl.ds(6 * lax.rem(chip, 2), 6)] = s

    def ag_wait(m):
        await_bytes(rsbuf.at[0, pl.ds(0, 15)], ag_r.at[m])
        send(scal.at[m], scal_o.at[m], fw_s.at[m], fw_r.at[m], mate)

    def fill(m):
        def one(t, carry):
            lanes = pl.ds(pl.multiple_of(t * 128, 128), 128)
            for e in range(HALF):
                inv = 1.0 / scal[m, e, t]
                blk = jnp.concatenate([xf[m, e, 0, :, lanes], xf[m, e, 1, :, lanes]], axis=0)
                tr[pl.ds(e, 128, stride=8), :] = (blk * inv).T
            sb[m, pl.ds(t * 128, 128)] = tr[...].reshape(128, 8, 128).astype(BF16)
            return carry

        lax.fori_loop(0, TILES, one, 0)

    def raw_fill():
        def one(t, carry):
            lanes = pl.ds(pl.multiple_of(t * 128, 128), 128)
            for e in range(HALF):
                blk = jnp.concatenate([xf[0, e, core, :, lanes], xo[0, e, :, lanes]], axis=0)
                tr[pl.ds(e, 128, stride=8), :] = blk.T
            rawsb[pl.ds(t * 128, 128)] = tr[...].reshape(128, 8, 128)
            return carry

        lax.fori_loop(0, TILES, one, 0)

    def raw_send():

        def go(to):
            send(rawsb.at[pl.ds(to * PIECE, RAW)], rraw.at[chip, core], rw_s.at[0], rw_r.at[0], to)

        for c in range(2):
            for dx, dy in OFFS:
                go(chip_at(dx, dy) * 2 + (core if c == 0 else 1 - core))
        go(mate)

    def raw_done(scale):
        rraw[chip, core] = rawsb[pl.ds(f * PIECE, RAW)]
        await_bytes(rawsb.at[pl.ds(0, 31 * RAW)], rw_r.at[0])
        inv = 1.0 / scale
        low = lax.broadcasted_iota(jnp.int32, (8, 128), 1) < 64

        def one(c, carry):
            lanes = pl.ds(pl.multiple_of(c * 128, 128), 128)
            for j in range(RAW):
                p, q = rraw[c, 0, j], rraw[c, 1, j]
                lo = jnp.where(low, p, q) * inv[:8, j:j + 1]
                hi = pltpu.roll(jnp.where(low, q, p), 64, 1) * inv[8:, j:j + 1]
                outs[0][j, :, lanes] = jnp.concatenate([lo, hi], axis=0).astype(BF16)
            return carry

        lax.fori_loop(0, 16, one, 0)

    def bulk(m):
        j0 = RAW if m == 0 else 0
        n = (PIECE - j0) // CUT

        def go(to, h):
            send(
                sb.at[m, pl.ds(to * PIECE + j0 + h * n, n)],
                outs[m].at[pl.ds(j0 + h * n, n), pl.ds(pl.multiple_of(core * 8, 8), 8), pl.ds(pl.multiple_of(chip * 128, 128), 128)],
                bk_s.at[m], bk_r.at[m], to)

        def turn(h, carry):
            for c in range(2):
                for dx, dy in OFFS:
                    go(chip_at(dx, dy) * 2 + (core if c == 0 else 1 - core), h)
            go(mate, h)
            return carry

        if m == 0:
            for h in range(CUT):
                turn(h, 0)
                swap(1 + h // 2, range(4 * (h % 2), 4 * (h % 2) + 4))
        else:
            lax.fori_loop(0, CUT, turn, 0)
        lanes = pl.ds(pl.multiple_of(chip * 128, 128), 128)
        for c in range(2):
            @pl.when(core == c)
            def _():
                def put(j, carry):
                    outs[m][j, 8 * c:8 * c + 8, lanes] = sb[m, f * PIECE + j]
                    return carry
                lax.fori_loop(j0, PIECE, put, 0)

    def route_pair():
        for c in rin:
            c.wait()
        v = rw[...] * gain[...]
        rhalf[0] = jnp.concatenate([v, v], axis=1)
        send(rhalf.at[0], rhalf.at[1], rt_s.at[0], rt_r.at[0], mate)

    def route_plane():
        await_bytes(rhalf.at[1], rt_r.at[0])
        low = lax.broadcasted_iota(jnp.int32, (EXP, 128), 1) < 64
        mine = low == (core == 0)
        rbuf[z, chip] = jnp.where(mine, rhalf[0], rhalf[1]).astype(BF16)
        for dx, dy in OFFS:
            send(rbuf.at[z, chip], rbuf.at[z, chip], rt_s.at[1], rt_r.at[1], chip_at(dx, dy) * 2 + core)

    def route_line():
        await_bytes(rbuf.at[0, pl.ds(0, 15)], rt_r.at[1])
        for dz in range(1, NZ):
            pltpu.make_async_remote_copy(
                src_ref=rbuf.at[z], dst_ref=rbuf.at[z], send_sem=rt_s.at[2], recv_sem=rt_r.at[2],
                device_id={"ep": lax.rem(z + dz, NZ)}, device_id_type=MESH).start()

    def route_out():
        await_bytes(rbuf.at[pl.ds(0, 3)], rt_r.at[2])
        for a in range(NZ):
            for c in range(16):
                rout[a * EXP:(a + 1) * EXP, c * 128:(c + 1) * 128] = rbuf[a, c]

    def scale_out(m):
        await_bytes(scal_o.at[m], fw_r.at[m])
        for e in range(HALF):
            for t in range(TILES + 1):
                own, oth = scal[m, e, t], scal_o[m, e, t]
                big[e:e + 1, t * 128:(t + 1) * 128] = jnp.where(core == 0, own, oth)
                big[HALF + e:HALF + e + 1, t * 128:(t + 1) * 128] = jnp.where(core == 0, oth, own)
        start = f * PIECE
        t0, r = lax.div(start, 128), lax.rem(start, 128)
        a = big[:, pl.ds(pl.multiple_of(t0 * 128, 128), 128)]
        b = big[:, pl.ds(pl.multiple_of(t0 * 128 + 128, 128), 128)]
        shift = lax.rem(128 - r, 128)
        a, b = pltpu.roll(a, shift, 1), pltpu.roll(b, shift, 1)
        lane = lax.broadcasted_iota(jnp.int32, (EXP, 128), 1)
        got = jnp.where(lane < 128 - r, a, b)
        scs[m][...] = got[:, :PIECE]
        return got

    for m in range(3):
        lax.fori_loop(0, HALF, functools.partial(sums, m), 0)
        if m == 0:
            pl.semaphore_wait(bar, 31 + NZ - 1)
        rs_send(m)
        if m == 0:
            swap(0)
    route_pair()
    raw_fill()
    ag_send(0)
    raw_send()
    ag_send(1)
    ag_send(2)
    route_plane()
    for m in range(3):
        ag_wait(m)
        await_bytes(xo.at[m], dsem_r.at[m])
        fill(m)
        bulk(m)
        if m == 0:
            route_line()
    scale = scale_out(0)
    raw_done(scale)
    for m in (1, 2):
        scale_out(m)
    route_out()
    await_bytes(rawsb.at[pl.ds(0, 31 * RAW)], rw_s.at[0])

    for m in range(3):
        await_bytes(xo.at[m], dsem_s.at[m])
        await_bytes(rsbuf.at[m], rs_s.at[m])
        await_bytes(rsbuf.at[0, pl.ds(0, 15)], ag_s.at[m])
        await_bytes(scal.at[m], fw_s.at[m])
    await_bytes(rhalf.at[0], rt_s.at[0])
    await_bytes(rbuf.at[0, pl.ds(0, 15)], rt_s.at[1])
    await_bytes(rbuf.at[pl.ds(0, 3)], rt_s.at[2])
    for m in range(3):
        size = 31 * (PIECE - RAW if m == 0 else PIECE)
        await_bytes(sb.at[m, pl.ds(0, size)], bk_s.at[m])
        await_bytes(sb.at[m, pl.ds(0, size)], bk_r.at[m])


def settle(*refs):
    n = len(refs) // 2
    sem = refs[-1]
    for i in range(n):
        pltpu.make_async_copy(refs[i], refs[n + i], sem.at[i]).start()
    for i in range(n):
        pltpu.make_async_copy(refs[i], refs[n + i], sem.at[i]).wait()


def body(train_gate, train_up, train_down, router_weight, router_gain):
    down = jnp.transpose(train_down, (0, 2, 1))
    shapes = (
        [jax.ShapeDtypeStruct((PIECE, EXP, 2048), BF16)] * 3
        + [jax.ShapeDtypeStruct((EXP, PIECE), F32)] * 3
        + [jax.ShapeDtypeStruct((EXP * NZ, 2048), BF16)]
    )
    vmem = pl.BlockSpec(memory_space=pltpu.VMEM)
    hbm = pl.BlockSpec(memory_space=pl.ANY)
    dma = pltpu.SemaphoreType.DMA
    got = pl.pallas_call(
        exchange,
        out_shape=shapes,
        in_specs=[hbm] * 5,
        out_specs=[vmem] * 7,
        scratch_shapes=[
            pltpu.VMEM((3, HALF, 2, ROWS, COLS), F32),
            pltpu.VMEM((3, HALF, ROWS, COLS), F32),
            pltpu.VMEM((6, HALF, TILES + 1, 1, 128), F32),
            pltpu.VMEM((3, 31, 6, 1, 128), F32),
            pltpu.VMEM((3, 6, 1, 128), F32),
            pltpu.VMEM((3, HALF, TILES + 1, 1, 128), F32),
            pltpu.VMEM((3, HALF, TILES + 1, 1, 128), F32),
            pltpu.VMEM((1024, 128), F32),
            pltpu.VMEM((3, COLS, 8, 128), BF16),
            pltpu.VMEM((COLS, 8, 128), F32),
            pltpu.VMEM((16, 2, RAW, 8, 128), F32),
            pltpu.VMEM((EXP, (TILES + 1) * 128), F32),
            pltpu.VMEM((EXP, ROWS), F32),
            pltpu.VMEM((1, ROWS), F32),
            pltpu.VMEM((2, EXP, 128), F32),
            pltpu.VMEM((NZ, 16, EXP, 128), BF16),
            dma((2,)), dma((3, HALF)), dma((3, HALF)), *[dma((3,))] * 12, dma((1,)), dma((1,)),
        ],
        compiler_params=pltpu.CompilerParams(
            collective_id=0, has_side_effects=True, vmem_limit_bytes=44 * 1024 * 1024
        ),
        name="exchange",
    )(train_gate, train_up, down, router_weight.T, router_gain[None, :])
    done = pl.pallas_call(
        settle,
        out_shape=shapes,
        in_specs=[vmem] * 7,
        out_specs=[hbm] * 7,
        scratch_shapes=[dma((7,))],
        compiler_params=pltpu.CompilerParams(vmem_limit_bytes=2 * 1024 * 1024),
        name="settle",
    )(*got)
    g, u, d, sg, su, sd, r = done
    back = lambda a: jnp.transpose(a, (1, 2, 0))
    return back(g), back(u), jnp.transpose(d, (1, 0, 2)), sg, su, sd, r.T


def solution(mesh):
    return jax.shard_map(
        body,
        mesh=mesh,
        in_specs=(
            P("ep", "fsdp", None),
            P("ep", "fsdp", None),
            P("ep", None, "fsdp"),
            P("fsdp", "ep"),
            P("fsdp"),
        ),
        out_specs=(
            P("ep", None, "fsdp"),
            P("ep", None, "fsdp"),
            P("ep", "fsdp", None),
            P("ep", "fsdp"),
            P("ep", "fsdp"),
            P("ep", "fsdp"),
            P(),
        ),
        check_vma=False,
    )
```
